32 devices in a mesh: row: 8 (over z, core), col: 4 (over y, x).
Axes of the slice: x: 2, y: 2, z: 4, core: 2. Of those that a mesh axis runs over, the one named last changes fastest.
Arguments:
- signal: float32 [128, 128, 256], P(None, 'row', 'col'), may hold values from -6 to 6
- symbol_x: float32 [128], replicated, may hold values from 0.3 to 3
- symbol_y: float32 [128], replicated, may hold values from 0.3 to 3
- symbol_z: float32 [256], replicated, may hold values from 0.3 to 3
Outputs:
- modes: float32 [128, 128, 256], P('row', 'col')
The draws below stay inside these ranges and needn't reach their ends.
All inputs are finite; a program needn't handle non-finite values.
Results may differ from the reference program's by a relative error of at most 0.0003.
Values sent between devices are 32-bit elements.
A program may use at most 64 MiB of HBM per device.

```python
import jax
import jax.numpy as jnp
from jax import lax

GRID_X = 128
GRID_Y = 128
GRID_Z = 256


def block_levels(key, dims, pieces, least, largest):
    gain = 1.0
    for dim, shards_of in pieces:
        steps = jax.random.uniform(jax.random.fold_in(jax.random.fold_in(key, 6), dim), (shards_of,), jnp.float32, least / len(pieces), largest / len(pieces))
        gain = gain * jnp.repeat(jnp.exp(steps), dims[dim] // shards_of).reshape((-1,) + (1,) * (len(dims) - 1 - dim))
    return gain


def normal_values(rng, dims, deviation, most, shards=(), dtype=jnp.bfloat16):
    factor_of = block_levels(rng, dims, shards, -0.22, 0.18) if shards else 1.0
    entries = jax.random.normal(rng, dims, jnp.float32) * deviation * factor_of
    return jnp.minimum(jnp.maximum(entries, -most), most).astype(dtype)


def setup_inputs(seed: int = 0) -> dict:
    key_of = jax.random.split(jax.random.key(seed), 5)
    return {
        "signal": normal_values(key_of[0], (GRID_X, GRID_Y, GRID_Z), 1.0, 6.0, ((1, 8), (2, 4)), jnp.float32),
        "symbol_x": jnp.clip(jax.random.uniform(key_of[1], (GRID_X,), jnp.float32, 0.3, 3.0), 0.3, 3.0),
        "symbol_y": jnp.clip(jax.random.uniform(key_of[2], (GRID_Y,), jnp.float32, 0.3, 3.0), 0.3, 3.0),
        "symbol_z": jnp.clip(jax.random.uniform(key_of[3], (GRID_Z,), jnp.float32, 0.3, 3.0), 0.3, 3.0),
    }


def mode_table(count):
    rank = jnp.arange(count)
    angle = (2.0 * jnp.pi / count) * ((rank[:, None] * rank[None, :]) % count).astype(jnp.float32)
    return (jnp.cos(angle) + jnp.sin(angle)) * (count ** -0.5)


def transform_dim(values, dim):
    moved = jnp.tensordot(values, mode_table(values.shape[dim]), axes=([dim], [0]), precision=lax.Precision.HIGHEST)
    return jnp.moveaxis(moved, -1, dim)


def reference(signal, symbol_x, symbol_y, symbol_z):
    modes = signal
    modes = transform_dim(modes, 0)
    modes = transform_dim(modes, 1)
    modes = transform_dim(modes, 2)
    symbol = symbol_x[:, None, None] + symbol_y[None, :, None] + symbol_z[None, None, :]
    modes = modes * ((1.0 - 0.2 * symbol) / (1.0 + 0.2 * symbol))
    return modes
```

```python
import functools

import jax
import jax.numpy as jnp
import numpy as np
from jax import lax
from jax.experimental import pallas as pl
from jax.experimental.pallas import tpu as pltpu
from jax.sharding import PartitionSpec as P

MESH = pl.DeviceIdType.MESH
CHUNKS = 4


def mode_table(count):
    rank = np.arange(count, dtype=np.int64)
    angle = 2.0 * np.pi / count * (rank[:, None] * rank[None, :] % count)
    return ((np.cos(angle) + np.sin(angle)) * count ** (-0.5)).astype(np.float32)


def halves(table):
    high = table.astype(jnp.bfloat16)
    low = (table - high.astype(np.float32)).astype(jnp.bfloat16)
    return high, low


def split(values):
    high = values.astype(jnp.bfloat16)
    return high, (values - high.astype(jnp.float32)).astype(jnp.bfloat16)


def dot(a, b):
    return jnp.dot(a, b, preferred_element_type=jnp.float32)


def table_times(table_ref, values):
    rows = table_ref.shape[0] // 2
    high, low = split(values)
    both = dot(table_ref[...], high)
    return both[:rows] + both[rows:] + dot(table_ref[:rows], low)


def kernel(nr, nc, sx_ref, sy_ref, sz_ref, signal_ref, tx_ref, ty_ref, tzh_ref, tzl_ref, out_ref,
           sent, got, turned, lines, factor, spread, send_1, recv_1, send_2, recv_2):
    me_r, me_c = lax.axis_index("row"), lax.axis_index("col")
    dim_x, part_y, part_z = signal_ref.shape
    share_x, share_y, dim_z = out_ref.shape
    half = share_x // 2
    step = half // CHUNKS
    chips = nr // 2
    chip, core = me_r // 2, lax.rem(me_r, 2)
    far = chip >= chips // 2
    place = jnp.where(far, chips - 1 - chip, chip)

    def row_peer(index):
        if index == 0:
            return me_r + 1 - 2 * core
        ahead, other = 1 + (index - 1) // 2, (index - 1) % 2
        spot = lax.rem(place + ahead, chips)
        spot = jnp.where(far, chips - 1 - spot, spot)
        return spot * 2 + lax.rem(core + other, 2)

    row_peers = [row_peer(i) for i in range(nr - 1)]
    col_peers = [lax.rem(me_c + i, nc) for i in range(1, nc)]

    barrier = pltpu.get_barrier_semaphore()
    for peer in row_peers:
        pl.semaphore_signal(barrier, inc=1, device_id=(peer, me_c), device_id_type=MESH)
    for peer in col_peers:
        pl.semaphore_signal(barrier, inc=1, device_id=(me_r, peer), device_id_type=MESH)

    lane_half = part_y // 2
    pairs = dim_x // 2
    for q in range(0, lane_half, 2):
        many = min(2, lane_half - q)
        block = jnp.concatenate(
            [signal_ref[:, y, :] for i in range(many) for y in (q + i, q + i + lane_half)], axis=1)
        moved = table_times(tx_ref, block)
        for i in range(many):
            at = 2 * part_z * i
            first, second = moved[:pairs, at:at + 2 * part_z], moved[pairs:, at:at + 2 * part_z]
            sent[:, q + i, :] = jnp.concatenate([first[:, :part_z], second[:, :part_z]], axis=1)
            sent[:, q + i + lane_half, :] = jnp.concatenate([first[:, part_z:], second[:, part_z:]], axis=1)

    pl.semaphore_wait(barrier, nr - 1 + nc - 1)

    def row_copy(k, peer):
        return pltpu.make_async_remote_copy(
            src_ref=sent.at[pl.ds(peer * half + k * step, step)],
            dst_ref=got.at[pl.ds(k * step, step), pl.ds(me_r * part_y, part_y)],
            send_sem=send_1.at[k, peer], recv_sem=recv_1.at[k, me_r],
            device_id=(peer, me_c), device_id_type=MESH)

    def row_arrival(k, peer):
        return pltpu.make_async_remote_copy(
            src_ref=sent.at[pl.ds(peer * half + k * step, step)],
            dst_ref=got.at[pl.ds(k * step, step), pl.ds(peer * part_y, part_y)],
            send_sem=send_1.at[k, peer], recv_sem=recv_1.at[k, peer],
            device_id=(peer, me_c), device_id_type=MESH)

    def col_copy(k, peer):
        return pltpu.make_async_remote_copy(
            src_ref=turned.at[pl.ds(k * step, step), pl.ds(peer * share_y, share_y)],
            dst_ref=lines.at[me_c, pl.ds(k * step, step)],
            send_sem=send_2.at[k, peer], recv_sem=recv_2.at[k, me_c],
            device_id=(me_r, peer), device_id_type=MESH)

    def col_arrival(k, peer):
        return pltpu.make_async_remote_copy(
            src_ref=turned.at[pl.ds(k * step, step), pl.ds(peer * share_y, share_y)],
            dst_ref=lines.at[peer, pl.ds(k * step, step)],
            send_sem=send_2.at[k, peer], recv_sem=recv_2.at[k, peer],
            device_id=(me_r, peer), device_id_type=MESH)

    for k in range(CHUNKS):
        for peer in row_peers:
            row_copy(k, peer).start()

    got[:, pl.ds(pl.multiple_of(me_r * part_y, part_y), part_y), :] = sent[
        pl.ds(pl.multiple_of(me_r * half, half), half)]

    for i in range(share_y):
        spread[pl.ds(i, 1), :] = jnp.full((1, dim_z), sy_ref[me_c * share_y + i], jnp.float32)
    for i in range(share_x):
        symbol = (sx_ref[me_r * share_x + i] + spread[...]) + sz_ref[...]
        factor[i] = (1.0 - 0.2 * symbol) / (1.0 + 0.2 * symbol)

    def finish(k):
        for peer in col_peers:
            col_arrival(k, peer).wait_recv()
        parts = [lines[c, pl.ds(k * step, step)].reshape(step * share_y, 2 * part_z) for c in range(nc)]
        rows = jnp.concatenate(
            [jnp.concatenate([p[:, :part_z] for p in parts], axis=1),
             jnp.concatenate([p[:, part_z:] for p in parts], axis=1)], axis=0)
        high, low = split(rows)
        modes = dot(high, tzh_ref[...]) + (dot(low, tzh_ref[...]) + dot(high, tzl_ref[...]))
        modes = modes.reshape(2, step, share_y, dim_z)
        for side in range(2):
            at = pl.ds(side * half + k * step, step)
            out_ref[at] = modes[side] * factor[at]

    for k in range(CHUNKS):
        for peer in row_peers:
            row_arrival(k, peer).wait_recv()
        block = jnp.concatenate([got[k * step + j] for j in range(step)], axis=1)
        moved = table_times(ty_ref, block)
        for j in range(step):
            turned[k * step + j] = moved[:, 2 * part_z * j:2 * part_z * (j + 1)]
        for peer in col_peers:
            col_copy(k, peer).start()
        lines[me_c, pl.ds(k * step, step)] = turned[
            pl.ds(k * step, step), pl.ds(pl.multiple_of(me_c * share_y, share_y), share_y), :]
        if k > 0:
            finish(k - 1)
    finish(CHUNKS - 1)

    for k in range(CHUNKS):
        for peer in row_peers:
            row_copy(k, peer).wait_send()
        for peer in col_peers:
            col_copy(k, peer).wait_send()


def solution(mesh):
    nr, nc = mesh.shape["row"], mesh.shape["col"]

    def on_device(signal, symbol_x, symbol_y, symbol_z):
        dim_x, part_y, part_z = signal.shape
        dim_y, dim_z = part_y * nr, part_z * nc
        share_x, share_y = dim_x // nr, dim_y // nc
        half = share_x // 2
        order = np.arange(dim_x).reshape(nr, 2, half).transpose(1, 0, 2).reshape(-1)
        table_x = np.concatenate(halves(mode_table(dim_x)[order]), axis=0)
        table_y = np.concatenate(halves(mode_table(dim_y)), axis=0)
        table_zh, table_zl = halves(mode_table(dim_z))
        vmem, smem = pl.BlockSpec(memory_space=pltpu.VMEM), pl.BlockSpec(memory_space=pltpu.SMEM)
        wide = 2 * part_z
        return pl.pallas_call(
            functools.partial(kernel, nr, nc),
            out_shape=jax.ShapeDtypeStruct((share_x, share_y, dim_z), jnp.float32),
            in_specs=[smem, smem] + [vmem] * 6,
            out_specs=vmem,
            scratch_shapes=[
                pltpu.VMEM((nr * half, part_y, wide), jnp.float32),
                pltpu.VMEM((half, dim_y, wide), jnp.float32),
                pltpu.VMEM((half, dim_y, wide), jnp.float32),
                pltpu.VMEM((nc, half, share_y, wide), jnp.float32),
                pltpu.VMEM((share_x, share_y, dim_z), jnp.float32),
                pltpu.VMEM((share_y, dim_z), jnp.float32),
                pltpu.SemaphoreType.DMA((CHUNKS, nr)),
                pltpu.SemaphoreType.DMA((CHUNKS, nr)),
                pltpu.SemaphoreType.DMA((CHUNKS, nc)),
                pltpu.SemaphoreType.DMA((CHUNKS, nc)),
            ],
            compiler_params=pltpu.CompilerParams(
                collective_id=0, has_side_effects=True, vmem_limit_bytes=60 * 1024 * 1024),
        )(symbol_x, symbol_y, symbol_z.reshape(1, dim_z), signal,
          jnp.asarray(table_x), jnp.asarray(table_y), jnp.asarray(table_zh), jnp.asarray(table_zl))

    placed = (P(None, "row", "col"), P(), P(), P())
    return jax.shard_map(
        on_device, mesh=mesh, in_specs=placed, out_specs=P("row", "col", None), check_vma=False)
```

```python
import functools

import jax
import jax.numpy as jnp
import numpy as np
from jax import lax
from jax.experimental import pallas as pl
from jax.experimental.pallas import tpu as pltpu
from jax.sharding import PartitionSpec as P

MESH = pl.DeviceIdType.MESH
SIZES = (5, 3,)
CHUNKS = len(SIZES)
LIMIT_SPARE = 8 * 1024 * 1024


def mode_table(count):
    rank = np.arange(count, dtype=np.int64)
    angle = 2.0 * np.pi / count * (rank[:, None] * rank[None, :] % count)
    return ((np.cos(angle) + np.sin(angle)) * count ** (-0.5)).astype(np.float32)


def halves(table):
    high = table.astype(jnp.bfloat16)
    low = (table - high.astype(np.float32)).astype(jnp.bfloat16)
    return high, low


def split(values):
    high = values.astype(jnp.bfloat16)
    return high, (values - high.astype(jnp.float32)).astype(jnp.bfloat16)


def dot(a, b):
    return jnp.dot(a, b, preferred_element_type=jnp.float32)


def dot_rows(a, b):
    return lax.dot_general(a, b, (((1,), (1,)), ((), ())), preferred_element_type=jnp.float32)


def table_times(table_ref, values, product):
    rows = table_ref.shape[0] // 2
    high, low = split(values)
    both = product(table_ref[...], high)
    return both[:rows] + both[rows:] + product(table_ref[:rows], low)


def kernel(nr, nc, sx_ref, sy_ref, sz_ref, signal_far, tx_far, ty_far, tzh_far, tzl_far, out_far,
           signal_ref, tx_ref, ty_ref, tzh_ref, tzl_ref, out_ref,
           sent, got, turned, lines, factor, spread, send_1, recv_1, send_2, recv_2, in_sem, out_sem):
    me_r, me_c = lax.axis_index("row"), lax.axis_index("col")
    part_y, part_z, dim_x = signal_ref.shape
    share_x, share_y, dim_z = out_ref.shape
    half = share_x // 2
    starts = [half * sum(SIZES[:k]) // sum(SIZES) for k in range(CHUNKS + 1)]
    steps = [starts[k + 1] - starts[k] for k in range(CHUNKS)]
    chips = nr // 2
    chip, core = me_r // 2, lax.rem(me_r, 2)
    far = chip >= chips // 2
    place = jnp.where(far, chips - 1 - chip, chip)

    def row_peer(index):
        if index == 0:
            return me_r + 1 - 2 * core
        ahead, other = 1 + (index - 1) // 2, (index - 1) % 2
        spot = lax.rem(place + ahead, chips)
        spot = jnp.where(far, chips - 1 - spot, spot)
        return spot * 2 + lax.rem(core + other, 2)

    row_peers = [row_peer(i) for i in range(nr - 1)]
    col_peers = [lax.rem(me_c + i, nc) for i in range(1, nc)]

    loads = [
        pltpu.make_async_copy(far_ref, near_ref, in_sem.at[i])
        for i, (far_ref, near_ref) in enumerate(
            ((signal_far, signal_ref), (tx_far, tx_ref), (ty_far, ty_ref), (tzh_far, tzh_ref), (tzl_far, tzl_ref)))]
    for load in loads:
        load.start()

    barrier = pltpu.get_barrier_semaphore()
    for peer in row_peers:
        pl.semaphore_signal(barrier, inc=1, device_id=(peer, me_c), device_id_type=MESH)
    for peer in col_peers:
        pl.semaphore_signal(barrier, inc=1, device_id=(me_r, peer), device_id_type=MESH)

    loads[0].wait()
    loads[1].wait()
    lane_half = part_y // 2
    pairs = dim_x // 2
    for q in range(0, lane_half, 2):
        many = min(2, lane_half - q)
        block = jnp.concatenate(
            [signal_ref[y] for i in range(many) for y in (q + i, q + i + lane_half)], axis=0)
        moved = table_times(tx_ref, block, dot_rows)
        for i in range(many):
            at = 2 * part_z * i
            first, second = moved[:pairs, at:at + 2 * part_z], moved[pairs:, at:at + 2 * part_z]
            sent[:, q + i, :] = jnp.concatenate([first[:, :part_z], second[:, :part_z]], axis=1)
            sent[:, q + i + lane_half, :] = jnp.concatenate([first[:, part_z:], second[:, part_z:]], axis=1)

    pl.semaphore_wait(barrier, nr - 1 + nc - 1)

    def row_copy(k, peer):
        return pltpu.make_async_remote_copy(
            src_ref=sent.at[pl.ds(peer * half + starts[k], steps[k])],
            dst_ref=got.at[pl.ds(starts[k], steps[k]), pl.ds(me_r * part_y, part_y)],
            send_sem=send_1.at[k, peer], recv_sem=recv_1.at[k, me_r],
            device_id=(peer, me_c), device_id_type=MESH)

    def row_arrival(k, peer):
        return pltpu.make_async_remote_copy(
            src_ref=sent.at[pl.ds(peer * half + starts[k], steps[k])],
            dst_ref=got.at[pl.ds(starts[k], steps[k]), pl.ds(peer * part_y, part_y)],
            send_sem=send_1.at[k, peer], recv_sem=recv_1.at[k, peer],
            device_id=(peer, me_c), device_id_type=MESH)

    def col_copy(k, peer):
        return pltpu.make_async_remote_copy(
            src_ref=turned.at[pl.ds(starts[k], steps[k]), pl.ds(peer * share_y, share_y)],
            dst_ref=lines.at[me_c, pl.ds(starts[k], steps[k])],
            send_sem=send_2.at[k, peer], recv_sem=recv_2.at[k, me_c],
            device_id=(me_r, peer), device_id_type=MESH)

    def col_arrival(k, peer):
        return pltpu.make_async_remote_copy(
            src_ref=turned.at[pl.ds(starts[k], steps[k]), pl.ds(peer * share_y, share_y)],
            dst_ref=lines.at[peer, pl.ds(starts[k], steps[k])],
            send_sem=send_2.at[k, peer], recv_sem=recv_2.at[k, peer],
            device_id=(me_r, peer), device_id_type=MESH)

    for k in range(CHUNKS):
        for peer in row_peers:
            row_copy(k, peer).start()

    got[:, pl.ds(pl.multiple_of(me_r * part_y, part_y), part_y), :] = sent[
        pl.ds(pl.multiple_of(me_r * half, half), half)]

    for i in range(share_y):
        spread[pl.ds(i, 1), :] = jnp.full((1, dim_z), sy_ref[me_c * share_y + i], jnp.float32)
    for i in range(share_x):
        symbol = (sx_ref[me_r * share_x + i] + spread[...]) + sz_ref[...]
        factor[i] = (1.0 - 0.2 * symbol) / (1.0 + 0.2 * symbol)

    for load in loads[2:]:
        load.wait()

    def stores(k):
        for side in range(2):
            at = pl.ds(side * half + starts[k], steps[k])
            yield pltpu.make_async_copy(out_ref.at[at], out_far.at[at], out_sem.at[k, side])

    def finish(k):
        for peer in col_peers:
            col_arrival(k, peer).wait_recv()
        parts = [lines[c, pl.ds(starts[k], steps[k])].reshape(steps[k] * share_y, 2 * part_z) for c in range(nc)]
        rows = jnp.concatenate(
            [jnp.concatenate([p[:, :part_z] for p in parts], axis=1),
             jnp.concatenate([p[:, part_z:] for p in parts], axis=1)], axis=0)
        high, low = split(rows)
        modes = dot(high, tzh_ref[...]) + (dot(low, tzh_ref[...]) + dot(high, tzl_ref[...]))
        modes = modes.reshape(2, steps[k], share_y, dim_z)
        for side in range(2):
            at = pl.ds(side * half + starts[k], steps[k])
            out_ref[at] = modes[side] * factor[at]
        for store in stores(k):
            store.start()

    for k in range(CHUNKS):
        for peer in row_peers:
            row_arrival(k, peer).wait_recv()
        block = jnp.concatenate([got[starts[k] + j] for j in range(steps[k])], axis=1)
        moved = table_times(ty_ref, block, dot)
        for j in range(steps[k]):
            turned[starts[k] + j] = moved[:, 2 * part_z * j:2 * part_z * (j + 1)]
        for peer in col_peers:
            col_copy(k, peer).start()
        lines[me_c, pl.ds(starts[k], steps[k])] = turned[
            pl.ds(starts[k], steps[k]), pl.ds(pl.multiple_of(me_c * share_y, share_y), share_y), :]
        if k > 0:
            finish(k - 1)
    finish(CHUNKS - 1)

    for k in range(CHUNKS):
        for peer in row_peers:
            row_copy(k, peer).wait_send()
        for peer in col_peers:
            col_copy(k, peer).wait_send()
        for store in stores(k):
            store.wait()


def solution(mesh):
    nr, nc = mesh.shape["row"], mesh.shape["col"]

    def on_device(signal, symbol_x, symbol_y, symbol_z):
        dim_x, part_y, part_z = signal.shape
        dim_y, dim_z = part_y * nr, part_z * nc
        share_x, share_y = dim_x // nr, dim_y // nc
        half = share_x // 2
        order = np.arange(dim_x).reshape(nr, 2, half).transpose(1, 0, 2).reshape(-1)
        table_x = np.concatenate(halves(mode_table(dim_x)[order]), axis=0)
        table_y = np.concatenate(halves(mode_table(dim_y)), axis=0)
        table_zh, table_zl = halves(mode_table(dim_z))
        vmem, smem = pl.BlockSpec(memory_space=pltpu.VMEM), pl.BlockSpec(memory_space=pltpu.SMEM)
        far = pl.BlockSpec(memory_space=pltpu.HBM)
        result = pl.BlockSpec(memory_space=pl.ANY)
        wide = 2 * part_z
        tables = [jnp.asarray(t) for t in (table_x, table_y, table_zh, table_zl)]
        out_shape = (share_x, share_y, dim_z)
        limit = 7 * signal.size * 4 + sum(t.size * 2 for t in tables) + LIMIT_SPARE
        return pl.pallas_call(
            functools.partial(kernel, nr, nc),
            out_shape=jax.ShapeDtypeStruct(out_shape, jnp.float32),
            in_specs=[smem, smem, vmem] + [far] * 5,
            out_specs=result,
            scratch_shapes=[
                pltpu.VMEM((part_y, part_z, dim_x), jnp.float32),
                *[pltpu.VMEM(t.shape, t.dtype) for t in tables],
                pltpu.VMEM(out_shape, jnp.float32),
                pltpu.VMEM((nr * half, part_y, wide), jnp.float32),
                pltpu.VMEM((half, dim_y, wide), jnp.float32),
                pltpu.VMEM((half, dim_y, wide), jnp.float32),
                pltpu.VMEM((nc, half, share_y, wide), jnp.float32),
                pltpu.VMEM((share_x, share_y, dim_z), jnp.float32),
                pltpu.VMEM((share_y, dim_z), jnp.float32),
                pltpu.SemaphoreType.DMA((CHUNKS, nr)),
                pltpu.SemaphoreType.DMA((CHUNKS, nr)),
                pltpu.SemaphoreType.DMA((CHUNKS, nc)),
                pltpu.SemaphoreType.DMA((CHUNKS, nc)),
                pltpu.SemaphoreType.DMA((5,)),
                pltpu.SemaphoreType.DMA((CHUNKS, 2)),
            ],
            compiler_params=pltpu.CompilerParams(
                collective_id=0, has_side_effects=True, vmem_limit_bytes=60 * 1024 * 1024),
        )(symbol_x, symbol_y, symbol_z.reshape(1, dim_z), signal.transpose(1, 2, 0), *tables)

    placed = (P(None, "row", "col"), P(), P(), P())
    return jax.shard_map(
        on_device, mesh=mesh, in_specs=placed, out_specs=P("row", "col", None), check_vma=False)
```
